32 devices in a mesh: dp: 4 (over x, core), cls: 8 (over z, y).
Axes of the slice: x: 2, y: 2, z: 4, core: 2. Of those that a mesh axis runs over, the one named last changes fastest.
Arguments:
- centers: float32 [16384, 512], P('cls'), may hold values from -6 to 6
- momentum: float32 [16384, 512], P('cls'), may hold values from -6 to 6
- grad_rows: bfloat16 [131072, 512], P(('dp', 'cls')), may hold values from -5400 to 5400
- row_ids: int32 [131072], P(('dp', 'cls')), may hold values from -1 to 16383, as said below
Outputs:
- new_centers: float32 [16384, 512], P('cls')
- new_momentum: float32 [16384, 512], P('cls')
The draws below stay inside these ranges and needn't reach their ends.
Inputs may be any that keep to these rules, and one draw needn't show every extreme that they name: `row_ids`: slots of one device come in 8 blocks of 512; block o holds only rows o * 2048 to (o + 1) * 2048 - 1 or -1; within a block the used slots come first, distinct and ascending, and one to 512 of them are used. In every draw, for some owner o, every device of some index of dp fills its whole block o.
All inputs are finite; a program needn't handle non-finite values.
Results may differ from the reference program's by a relative error of at most 0.0003.
Values may be sent and summed in bfloat16 or wider, within the bound.
No kernel may reach another device: no remote copies, remote signals or barrier semaphores. Data moves between devices by JAX's collectives and lax.ppermute only.
A program may use at most 128 MiB of HBM per device.

```python
import math
import jax
import jax.numpy as jnp
from jax import lax

D = 512
ROWS_DEV = 2048
SAMP_DEV = 4096
CLASSES = 16384
N_DP = 4
N_CLS = 8


def draw_row_ids(key, part):
    capacity = SAMP_DEV // N_CLS
    subkeys = jax.random.split(jax.random.fold_in(key, 11), 3)
    counts = jax.random.randint(subkeys[0], (N_DP, N_CLS, N_CLS), max(capacity // 3, 1), capacity + 1)
    full_owner = jax.random.randint(subkeys[1], (N_DP,), 0, N_CLS)
    owner_line = jnp.arange(N_CLS, dtype=jnp.int32)
    counts = jnp.where(owner_line[None, None, :] == full_owner[:, None, None], capacity, counts)
    scores = jax.random.randint(subkeys[2], (N_DP, N_CLS, N_CLS, ROWS_DEV), 0, 2 ** 30 // ROWS_DEV)
    scores = scores * ROWS_DEV + jnp.arange(ROWS_DEV, dtype=jnp.int32)
    unused, picked = lax.top_k(scores, capacity)
    living = jnp.arange(capacity, dtype=jnp.int32)[None, None, None, :] < counts[..., None]
    ordered_key = jnp.sort(jnp.where(living, picked, ROWS_DEV), axis=-1)
    owner_rows = owner_line[None, None, :, None] * ROWS_DEV
    result = jnp.where(ordered_key < ROWS_DEV, ordered_key + owner_rows, -1)
    return result.reshape(-1).astype(jnp.int32)


def draw_grad_rows(key, part):
    capacity = SAMP_DEV // N_CLS
    subkeys = jax.random.split(jax.random.fold_in(key, 23), 3)
    shape = (N_DP, N_CLS, N_CLS, capacity, D)
    base = jnp.clip(jax.random.normal(subkeys[0], shape, jnp.float32), -6.0, 6.0)
    row_scale = jnp.exp(jax.random.uniform(subkeys[1], (N_DP, N_CLS, N_CLS, capacity, 1), jnp.float32, 0.0, math.log(10.0)))
    col_scale = jnp.exp(jax.random.uniform(subkeys[2], (D,), jnp.float32, 0.0, math.log(10.0)))
    owner_ramp = 3.0 ** (jnp.arange(N_CLS, dtype=jnp.float32) / (N_CLS - 1))
    replica_ramp = 3.0 ** (jnp.arange(N_DP, dtype=jnp.float32) / max(N_DP - 1, 1))
    ramps = replica_ramp[:, None, None, None, None] * owner_ramp[None, None, :, None, None]
    values = base * row_scale * col_scale * ramps
    return values.reshape(N_DP * N_CLS * SAMP_DEV, D).astype(jnp.bfloat16)


def level_of(stream_key, extent, shards, least, high):
    level, own = 1.0, jax.random.fold_in(stream_key, 6)
    for axis_at, shards_of in shards:
        heights = jnp.exp(jax.random.uniform(jax.random.fold_in(own, axis_at), (shards_of,), jnp.float32, least / len(shards), high / len(shards)))
        level = level * jnp.repeat(heights, extent[axis_at] // shards_of).reshape([-1 if axis == axis_at else 1 for axis in range(len(extent))])
    return level


def normal_values(own_key, dims, spread, most, cuts=(), held_as=jnp.bfloat16):
    array = jax.random.normal(own_key, dims, jnp.float32) * spread
    if len(cuts) > 0:
        array = level_of(own_key, dims, cuts, -0.22, 0.18) * array
    return jnp.clip(array, min=-most, max=most).astype(held_as)


def setup_inputs(seed: int = 0) -> dict:
    splits = jax.random.split(jax.random.key(seed), 5)
    centers = normal_values(splits[0], (CLASSES, D), 1.0, 6.0, ((0, 8),), jnp.float32)
    momentum = normal_values(splits[1], (CLASSES, D), 1.0, 6.0, ((0, 8),), jnp.float32)
    grad_rows = draw_grad_rows(jax.random.fold_in(splits[4], 71), 0)
    row_ids = draw_row_ids(jax.random.fold_in(splits[4], 71), 0)
    return dict(centers=centers, momentum=momentum, grad_rows=grad_rows, row_ids=row_ids)


beta_decay = 0.9
learn_rate = 0.5
clip_rms = 1.0
eps_norm = 1e-06
eps_row = 1e-06

def reference(centers, momentum, grad_rows, row_ids):
    targets = jnp.where(row_ids >= 0, row_ids, CLASSES).astype(jnp.int32)
    gradient = jnp.zeros((CLASSES, D), jnp.float32).at[targets].add(grad_rows.astype(jnp.float32), mode='drop')
    squares = jnp.sum(gradient * gradient)
    ceiling = clip_rms * math.sqrt(CLASSES * D)
    factor = jnp.minimum(1.0, ceiling / jnp.sqrt(squares + eps_norm))
    new_momentum = beta_decay * momentum + factor * gradient
    stepped = centers - learn_rate * new_momentum
    rescale = lax.rsqrt(lax.optimization_barrier(jnp.mean(stepped * stepped, axis=1, keepdims=True)) + eps_row)
    return (stepped * rescale, new_momentum)
```

```python
import functools
import math

import jax
import jax.numpy as jnp
from jax import lax
from jax.experimental import pallas as pl
from jax.experimental.pallas import tpu as pltpu
from jax.sharding import PartitionSpec as P

beta_decay = 0.9
learn_rate = 0.5
clip_rms = 1.0
eps_norm = 1e-06
eps_row = 1e-06

PIECES = 2
INTERPRET = False


def scatter_kernel(n_rows_in, tile, cap, ids_ref, *refs):
    row_refs, out_ref = refs[:n_rows_in], refs[n_rows_in]
    first = pl.program_id(0) * tile
    line = first + lax.broadcasted_iota(jnp.int32, (tile, cap), 0)
    total = None
    at = 0
    for ref in row_refs:
        for s in range(ref.shape[0] // cap):
            ids = ids_ref[pl.ds(at, 1), :]
            table = jnp.where(line == ids, 1.0, 0.0).astype(jnp.bfloat16)
            part = jnp.dot(table, ref[s * cap:(s + 1) * cap, :], preferred_element_type=jnp.float32)
            total = part if total is None else total + part
            at += 1
    out_ref[...] = total


def scatter_rows(ids, rows, n_out):
    cap, width = ids.shape[1], rows[0].shape[1]
    tile = math.gcd(n_out, 256)
    flops = 2 * n_out * ids.size * width
    return pl.pallas_call(
        functools.partial(scatter_kernel, len(rows), tile, cap),
        grid=(n_out // tile,),
        in_specs=[pl.BlockSpec(ids.shape, lambda i: (0, 0))] + [pl.BlockSpec(r.shape, lambda i: (0, 0)) for r in rows],
        out_specs=pl.BlockSpec((tile, width), lambda i: (i, 0)),
        out_shape=jax.ShapeDtypeStruct((n_out, width), jnp.float32),
        cost_estimate=pl.CostEstimate(flops=flops, bytes_accessed=4 * n_out * width, transcendentals=0),
        interpret=INTERPRET,
        name="scatter_rows",
    )(ids, *rows)


def update_kernel(n, width, slot_ref, factor_ref, c_ref, m_ref, *refs):
    g_refs, (newc_ref, newm_ref) = refs[:n], refs[n:]
    factor = factor_ref[0, 0]
    for k in range(n):
        cols = pl.ds(pl.multiple_of(slot_ref[0, k] * width, width), width)
        moved = beta_decay * m_ref[:, cols] + factor * g_refs[k][...]
        newm_ref[:, cols] = moved
        stepped = c_ref[:, cols] - learn_rate * moved
        newc_ref[:, cols] = stepped
    stepped = newc_ref[...]
    mean = jnp.sum(stepped * stepped, axis=1, keepdims=True) * (1.0 / (n * width))
    newc_ref[...] = stepped * lax.rsqrt(mean + eps_row)


def update(slots, factor, centers, momentum, parts):
    rows, features = centers.shape
    width = parts[0].shape[1]
    n = len(parts)
    tile = math.gcd(rows, 256)
    whole = pl.BlockSpec((tile, features), lambda i: (i, 0))
    return pl.pallas_call(
        functools.partial(update_kernel, n, width),
        grid=(rows // tile,),
        in_specs=[
            pl.BlockSpec(memory_space=pltpu.SMEM),
            pl.BlockSpec(memory_space=pltpu.SMEM),
            whole,
            whole,
        ] + [pl.BlockSpec((tile, width), lambda i: (i, 0))] * n,
        out_specs=[whole, whole],
        out_shape=[jax.ShapeDtypeStruct(centers.shape, jnp.float32)] * 2,
        cost_estimate=pl.CostEstimate(flops=10 * rows * features, bytes_accessed=20 * rows * features, transcendentals=0),
        interpret=INTERPRET,
        name="update_rows",
    )(slots, factor, centers, momentum, *parts)


def on_device(X, Z, Y, centers, momentum, grad_rows, row_ids):
    C = 2
    DP, CLS = X * C, Z * Y
    rows_dev, features = centers.shape
    cap = grad_rows.shape[0] // CLS
    F = features // DP
    dp, cl = lax.axis_index("dp"), lax.axis_index("cls")
    x, c, z, y = dp // C, dp % C, cl // Y, cl % Y
    bf16 = jnp.bfloat16

    def send(a, move):
        pairs = []
        for i in range(DP * CLS):
            d, k = divmod(i, CLS)
            to = move(d // C, d % C, k // Y, k % Y)
            if to is not None:
                tx, tc, tz, ty = to
                pairs.append((i, (tx * C + tc) * CLS + tz * Y + ty))
        return lax.ppermute(a, ("dp", "cls"), pairs)

    other_core = lambda x, c, z, y: (x, 1 - c, z, y)
    offsets = [(dx, dy) for dx in range(X) for dy in range(Y) if (dx, dy) != (0, 0)]

    def shift(dx, dy):
        return lambda x, c, z, y: ((x + dx) % X, c, z, (y + dy) % Y)

    right = lambda h, d=None: (lambda x, c, z, y: (x, c, z + h, y) if z + (d or h) < Z else None)
    left = lambda h, d=None: (lambda x, c, z, y: (x, c, z - h, y) if z - (d or h) >= 0 else None)

    plane = Y * cap

    def rows_of(t):
        t = jnp.clip(t, 0, Z - 1)
        return lax.dynamic_slice(grad_rows, (t * plane, 0), (plane, features))

    from_left = send(rows_of(z + 1), right(1))
    from_right = send(rows_of(z - 1), left(1))

    owner_first = lax.broadcasted_iota(jnp.int32, (CLS, cap), 0) * rows_dev
    sent_ids = row_ids.reshape(CLS, cap)
    own_ids = jnp.where(sent_ids >= 0, sent_ids - owner_first, -1)
    pair_ids = jnp.stack([own_ids, send(own_ids, other_core)])
    plane_ids = [pair_ids] + [send(pair_ids, shift(dx, dy)) for dx, dy in offsets]
    plane_ids = jnp.concatenate(plane_ids).reshape(-1, Z, Y, cap)

    def ids_for(t):
        got = lax.dynamic_slice(plane_ids, (0, jnp.clip(t, 0, Z - 1), y, 0), (plane_ids.shape[0], 1, 1, cap))
        return got.reshape(-1, cap)

    def cut(src, r0, d, n):
        return lax.dynamic_slice(src, (r0, d * F), (n, F))

    def exchange(sources):
        out = jnp.stack([jnp.stack([cut(a, r, i * C + (1 - c), plane) for i in range(X)]) for a, r in sources])
        got = send(out, other_core)

        def payload(px, py):
            both = []
            for u, (a, r) in enumerate(sources):
                both.append(cut(a, r + py * cap, px * C + c, cap))
                both.append(lax.dynamic_slice(got, (u, px, py * cap, 0), (1, 1, cap, F)).reshape(cap, F))
            return jnp.concatenate(both)

        outs = [payload(x, y)]
        for dx, dy in offsets:
            outs.append(send(payload((x + dx) % X, (y + dy) % Y), shift(dx, dy)))
        return outs

    def far(t):
        t = jnp.clip(t, 0, Z - 1)
        got = exchange([(grad_rows, t * plane)])
        return scatter_rows(ids_for(t), got, rows_dev)

    def pieces(a):
        n = a.shape[0] // PIECES
        return [a[i * n:(i + 1) * n] for i in range(PIECES)]

    add = lambda a, b: [p if q is None else p + q for p, q in zip(a, b)]
    none = [None] * PIECES
    carry_r, carry_l = none, none
    for d in range(Z - 1, 1, -1):
        hop = 1 if d > 2 else 2
        if 2 * d >= Z:
            t = jnp.where(z + d < Z, z + d, z - d)
            unit = add(add(pieces(far(t)), carry_r), carry_l)
            ends = [p + hop for p in range(Z - d)] + [p - hop for p in range(d, Z)]
            if len(set(ends)) == len(ends):

                def both(x, c, z, y, d=d, hop=hop):
                    return right(hop, d)(x, c, z, y) or left(hop, d)(x, c, z, y)

                got = [send(u, both) for u in unit]
                came_right = (z >= hop) & (z - hop + d < Z)
                got_r, got_l = got, none
                if d > 2 and 2 * (d - 1) < Z:
                    got_r = [jnp.where(came_right, q, 0) for q in got]
                    got_l = [jnp.where(came_right, 0, q) for q in got]
            else:
                got_r = [send(u, right(hop, d)) for u in unit]
                got_l = [send(u, left(hop, d)) for u in unit]
        else:
            go_r = add(pieces(far(z + d)), carry_r)
            go_l = add(pieces(far(z - d)), carry_l)
            got_r = [send(u, right(hop, d)) for u in go_r]
            got_l = [send(u, left(hop, d)) for u in go_l]
        carry_r, carry_l = got_r, got_l
    arrived = add(carry_r, carry_l) if carry_r is not none else none

    left_ids = send(ids_for(z + 1), right(1))
    right_ids = send(ids_for(z - 1), left(1))
    none_l = jnp.where(z > 0, left_ids, -1)
    none_r = jnp.where(z < Z - 1, right_ids, -1)
    near = exchange([(grad_rows, z * plane), (from_left, 0), (from_right, 0)])
    near_ids = jnp.stack([
        ids_for(z).reshape(-1, 2, cap), none_l.reshape(-1, 2, cap), none_r.reshape(-1, 2, cap)
    ], axis=1).reshape(-1, cap)
    near_sum = pieces(scatter_rows(near_ids, near, rows_dev))
    share = add(near_sum, arrived)

    total = jnp.zeros((1, 128), jnp.float32)
    for s in share:
        total = total + jnp.sum(s * s)
    total = total + send(total, other_core)
    k = 1
    while k < X:
        total = total + send(total, lambda x, c, z, y: (x ^ k, c, z, y))
        k *= 2
    k = 1
    while k < Y:
        total = total + send(total, lambda x, c, z, y: (x, c, z, y ^ k))
        k *= 2
    k = 1
    while k < Z:
        total = total + send(total, lambda x, c, z, y: (x, c, z ^ k, y))
        k *= 2
    squares = total[:, :1]
    ceiling = clip_rms * math.sqrt(rows_dev * CLS * features)
    factor = jnp.minimum(1.0, ceiling / jnp.sqrt(squares + eps_norm))

    parts, slots = [[] for _ in range(DP)], []
    for s in share:
        mine = [s] + [send(s, shift(dx, 0)) for dx in range(1, X)]
        for i, a in enumerate(mine):
            parts[2 * i].append(a)
            parts[2 * i + 1].append(send(a, other_core))
    for dx in range(X):
        from_x = (x - dx) % X
        slots += [from_x * C + c, from_x * C + (1 - c)]
    parts = [jnp.concatenate(p) for p in parts]
    if F % 128 == 0:
        slots = jnp.stack(slots).astype(jnp.int32).reshape(1, DP)
        return tuple(update(slots, factor, centers, momentum, parts))
    gradient = jnp.zeros((rows_dev, features), jnp.float32)
    for s, p in zip(slots, parts):
        gradient = lax.dynamic_update_slice(gradient, p, (0, s * F))
    new_momentum = beta_decay * momentum + factor * gradient
    stepped = centers - learn_rate * new_momentum
    rescale = lax.rsqrt(jnp.mean(stepped * stepped, axis=1, keepdims=True) + eps_row)
    return (stepped * rescale, new_momentum)


def solution(mesh):
    replicas, groups = mesh.shape["dp"], mesh.shape["cls"]
    Y = 1
    while groups % (4 * Y) == 0 and 2 * (2 * Y) * (2 * Y) <= groups:
        Y *= 2
    placed = (P("cls", None), P("cls", None), P(("dp", "cls"), None), P(("dp", "cls")))
    return jax.shard_map(
        functools.partial(on_device, replicas // 2, groups // Y, Y),
        mesh=mesh,
        in_specs=placed,
        out_specs=(P("cls", None), P("cls", None)),
        check_vma=False,
    )
```
